256 devices in a mesh: emb: 16 (over z, core), dp: 16 (over x, y).
Axes of the slice: x: 4, y: 4, z: 8, core: 2. Of those that a mesh axis runs over, the one named last changes fastest.
Arguments:
- embeddings: bfloat16 [512, 1024, 256], P('emb', 'dp'), may hold values from -9 to 9
- machine_projection: bfloat16 [512, 32], replicated, may hold values from -0.015625 to 0.015625
- w_lcb: bfloat16 [512, 512], P('dp'), may hold values from -0.25 to 0.25
- w_fmb: bfloat16 [32, 256], replicated, may hold values from -1 to 1
- ln_gain: float32 [512, 256], P('emb'), may hold values from 0.5 to 1.5
- ln_bias: float32 [512, 256], P('emb'), may hold values from -1.8 to 1.8
Outputs:
- layer_out: bfloat16 [512, 1024, 256], P('emb', 'dp')
The draws below stay inside these ranges and needn't reach their ends.
All inputs are finite; a program needn't handle non-finite values.
Results may differ from the reference program's by a relative error of at most 0.007.
Values may be sent and summed in bfloat16 or wider, within the bound.
A program may use at most 64 MiB of HBM per device.

```python
import jax
import jax.numpy as jnp
from jax import lax

N = 512
D = 256
K = 32
B = 1024


def draw_embeddings(key, part):
    noise_key = jax.random.fold_in(key, 11)
    sample_key = jax.random.fold_in(key, 12)
    position = jnp.arange(N, dtype=jnp.float32) / jnp.float32(max(N - 1, 1))
    sample_scale = jnp.exp(jax.random.uniform(sample_key, (B,), jnp.float32, jnp.log(0.5), jnp.log(2.0)))
    noise = jnp.clip(jax.random.normal(noise_key, (N, B, D), jnp.float32), -6.0, 6.0)
    offset = 0.3 * jnp.exp(position * jnp.log(3.0))
    values = noise + offset[:, None, None] * sample_scale[None, :, None]
    return values.astype(jnp.bfloat16)


def level_of(rng, dims, pieces, smallest, top_value):
    def one(dim, blocks):
        heights = jax.random.uniform(jax.random.fold_in(jax.random.fold_in(rng, 6), dim), (blocks,), jnp.float32, smallest / len(pieces), top_value / len(pieces))
        return jnp.repeat(jnp.exp(heights), dims[dim] // blocks).reshape((-1,) + (1,) * (len(dims) - dim - 1))

    gain = one(*pieces[0])
    for cut in pieces[1:]:
        gain = gain * one(*cut)
    return gain


def gaussian(stream_key, dims, scale, bound, pieces=(), held_as=jnp.bfloat16):
    drawn = scale * jax.random.normal(stream_key, dims, jnp.float32)
    if pieces:
        drawn = drawn * level_of(stream_key, dims, pieces, -0.22, 0.18)
    return jnp.clip(drawn, -bound, bound).astype(held_as)


def setup_inputs(seed: int = 0) -> dict:
    key_list = jax.random.split(jax.random.key(seed), 7)
    embeddings = draw_embeddings(jax.random.fold_in(key_list[6], 71), 0)
    machine_projection = gaussian(key_list[1], (N, K), (N * D) ** -0.5, 0.015625)
    w_lcb = gaussian(key_list[2], (N, N), N ** -0.5, 0.25, ((0, 16),))
    w_fmb = gaussian(key_list[3], (K, D), K ** -0.5, 1.0)
    ln_gain = jnp.clip(1.0 + 0.1 * jax.random.normal(key_list[4], (N, D), jnp.float32), 0.5, 1.5)
    ln_bias = gaussian(key_list[5], (N, D), 0.3, 1.8, ((0, 16),), jnp.float32)
    return dict(embeddings=embeddings, machine_projection=machine_projection, w_lcb=w_lcb, w_fmb=w_fmb, ln_gain=ln_gain, ln_bias=ln_bias)


def reference(embeddings, machine_projection, w_lcb, w_fmb, ln_gain, ln_bias):
    emb_count, samples, width = embeddings.shape
    factor_dimension = machine_projection.shape[1]
    compressed = jnp.dot(w_lcb, embeddings.reshape(emb_count, samples * width), preferred_element_type=jnp.float32).reshape(emb_count, samples, width)
    widened_inputs = embeddings.astype(jnp.float32)
    summed_values = jnp.einsum('slc,sf->lfc', widened_inputs, machine_projection.astype(jnp.float32))
    factor_matrix = summed_values.astype(jnp.bfloat16)
    inner_product = jnp.einsum('gue,ufe->guf', widened_inputs, factor_matrix.astype(jnp.float32)).astype(jnp.bfloat16)
    fmb_out = jnp.dot(inner_product.reshape(emb_count * samples, factor_dimension), w_fmb, preferred_element_type=jnp.float32).reshape(emb_count, samples, width)
    mixed = widened_inputs + compressed + fmb_out
    entries = jnp.float32(emb_count * width)
    average = lax.optimization_barrier(jnp.sum(mixed, axis=(0, 2))) / entries
    centered = mixed - average[None, :, None]
    spread = lax.optimization_barrier(jnp.sum(centered * centered, axis=(0, 2))) / entries
    scaled = centered * jax.lax.rsqrt(spread + 1e-05)[None, :, None]
    return (scaled * ln_gain[:, None, :] + ln_bias[:, None, :]).astype(jnp.bfloat16)
```

```python
import functools

import jax
import jax.numpy as jnp
from jax import lax
from jax.experimental import pallas as pl
from jax.experimental.pallas import tpu as pltpu
from jax.sharding import PartitionSpec as P

MESH = pl.DeviceIdType.MESH
PEERS = ((0, 1),) + tuple((d, c) for d in (1, 7, 2, 6, 3, 5, 4) for c in (0, 1))
PITCH = 24


def kernel(
    emb_ref, mp_ref, w_ref, wf_ref, g_ref, b_ref, out_ref,
    ebuf, stage, sendbuf, xbuf, wfull, rbuf, ybuf, mixed, wf_v, g_v, b_v,
    load_sem, small_sem, in_send, in_recv, out_send, out_recv, w_send, w_recv,
):
    e = lax.axis_index("emb")
    dp = lax.axis_index("dp")
    z, c = e // 2, e % 2
    rows, samples, width = ebuf.shape
    chunks, group = sendbuf.shape[0], sendbuf.shape[1]
    emb_count = xbuf.shape[1]
    n_dp = w_send.shape[0] + 1

    def peer(d, cc):
        return lax.rem(z + d, 8) * 2 + lax.rem(c + cc, 2)

    barrier = pltpu.get_barrier_semaphore()
    for d, cc in PEERS:
        pl.semaphore_signal(barrier, inc=1, device_id={"emb": peer(d, cc)}, device_id_type=MESH)
    for k in range(1, n_dp):
        pl.semaphore_signal(barrier, inc=1, device_id={"dp": lax.rem(dp + k, n_dp)}, device_id_type=MESH)

    def load(s):
        part = pl.ds(s * group, group)
        return pltpu.make_async_copy(emb_ref.at[:, part], ebuf.at[:, part], load_sem.at[s])

    my_w = pl.ds(pl.multiple_of(dp * rows, rows), rows)
    load(0).start()
    own_w = pltpu.make_async_copy(w_ref, wfull.at[my_w], small_sem.at[0])
    own_w.start()
    for s in range(1, chunks):
        load(s).start()
    small = [
        pltpu.make_async_copy(a, v, small_sem.at[1 + i])
        for i, (a, v) in enumerate(((mp_ref, wfull.at[pl.ds(emb_count, mp_ref.shape[0])]), (wf_ref, wf_v), (g_ref, g_v), (b_ref, b_v)))
    ]
    for copy in small:
        copy.start()

    my_rows = pl.ds(pl.multiple_of(e * rows, rows), rows)

    def prepare(s):
        load(s).wait()
        for n in range(rows):
            block = ebuf[n, pl.ds(pl.multiple_of(s * group, group), group), :].astype(jnp.float32)
            for h in range(2):
                stage[h, pl.ds(n * PITCH, group), :] = block[:, h * 128 : (h + 1) * 128]
        for b in range(group):
            for h in range(2):
                sendbuf[s, b, :, pl.ds(h * 128, 128)] = stage[h, pl.ds(b, rows, stride=PITCH), :].astype(jnp.bfloat16)
        xbuf[s, my_rows, :] = sendbuf[s, e]

    def send_in(s):
        for i, (d, cc) in enumerate(PEERS):
            j = peer(d, cc)
            pltpu.make_async_remote_copy(
                src_ref=sendbuf.at[s, j], dst_ref=xbuf.at[s, my_rows],
                send_sem=in_send.at[s], recv_sem=in_recv.at[s],
                device_id={"emb": j}, device_id_type=MESH,
            ).start()

    def w_copy(k):
        return pltpu.make_async_remote_copy(
            src_ref=wfull.at[my_w], dst_ref=wfull.at[my_w], send_sem=w_send.at[k - 1], recv_sem=w_recv,
            device_id={"dp": lax.rem(dp + k, n_dp)}, device_id_type=MESH,
        )

    prepare(0)
    own_w.wait()
    pl.semaphore_wait(barrier, len(PEERS) + n_dp - 1)
    send_in(0)
    for k in range(1, n_dp):
        w_copy(k).start()

    def feed(s, carry):
        prepare(s)
        send_in(s)
        return carry

    lax.fori_loop(1, chunks, feed, 0)

    for copy in small:
        copy.wait()
    others = pl.ds(0, emb_count - rows)
    pltpu.make_async_copy(wfull.at[others], wfull.at[others], w_recv).wait()

    block = 128
    entries = jnp.float32(emb_count * width)

    def mix(s, carry):
        pltpu.make_async_copy(xbuf.at[s, others], xbuf.at[s, others], in_recv.at[s]).wait()
        x = xbuf[s]
        factor = jnp.dot(wfull[pl.ds(emb_count, 32), :], x, preferred_element_type=jnp.float32).astype(jnp.bfloat16)
        total = jnp.zeros((8, width), jnp.float32)
        for i in range(emb_count // block):
            part = pl.ds(i * block, block)
            xb = xbuf[s, part, :]
            inner = lax.dot_general(xb, factor, (((1,), (1,)), ((), ())), preferred_element_type=jnp.float32).astype(jnp.bfloat16)
            m = jnp.dot(wfull[part, :], x, preferred_element_type=jnp.float32)
            m = m + xb.astype(jnp.float32) + jnp.dot(inner, wf_v[...], preferred_element_type=jnp.float32)
            mixed[part, :] = m
            total = total + jnp.sum(m.reshape(block // 8, 8, width), axis=0)
        average = jnp.sum(total, keepdims=True) / entries
        square = jnp.zeros((8, width), jnp.float32)
        for i in range(emb_count // block):
            centered = mixed[pl.ds(i * block, block), :] - average
            square = square + jnp.sum((centered * centered).reshape(block // 8, 8, width), axis=0)
        scale = lax.rsqrt(jnp.sum(square, keepdims=True) / entries + 1e-05)
        for i in range(emb_count // block):
            part = pl.ds(i * block, block)
            rbuf[s, part, :] = ((mixed[part, :] - average) * scale).astype(jnp.bfloat16)
        ybuf[s, e] = rbuf[s, my_rows, :]
        for i, (d, cc) in enumerate(PEERS):
            j = peer(d, cc)
            pltpu.make_async_remote_copy(
                src_ref=rbuf.at[s, pl.ds(pl.multiple_of(j * rows, rows), rows)], dst_ref=ybuf.at[s, e],
                send_sem=out_send.at[s], recv_sem=out_recv.at[s],
                device_id={"emb": j}, device_id_type=MESH,
            ).start()
        return carry

    lax.fori_loop(0, chunks, mix, 0)

    fifteen = pl.ds(0, group - 1)

    def finish(s, carry):
        pltpu.make_async_copy(ybuf.at[s, fifteen], ybuf.at[s, fifteen], out_recv.at[s]).wait()
        part = pl.ds(pl.multiple_of(s * group, group), group)
        for b in range(group):
            y = ybuf[s, b].astype(jnp.float32) * g_v[...] + b_v[...]
            for h in range(2):
                stage[h, pl.ds(b, rows, stride=PITCH), :] = y[:, h * 128 : (h + 1) * 128]
        for n in range(rows):
            for h in range(2):
                out_ref[n, part, pl.ds(h * 128, 128)] = stage[h, pl.ds(n * PITCH, group), :].astype(jnp.bfloat16)
        return carry

    lax.fori_loop(0, chunks, finish, 0)

    def drain(s, carry):
        pltpu.make_async_copy(sendbuf.at[s, fifteen], sendbuf.at[s, fifteen], in_send.at[s]).wait()
        pltpu.make_async_copy(ybuf.at[s, fifteen], ybuf.at[s, fifteen], out_send.at[s]).wait()
        return carry

    lax.fori_loop(0, chunks, drain, 0)
    for k in range(1, n_dp):
        w_copy(k).wait_send()


def body(embeddings, machine_projection, w_lcb, w_fmb, ln_gain, ln_bias):
    rows, samples, width = embeddings.shape
    emb_count, rank = machine_projection.shape
    group = emb_count // rows
    chunks = samples // group
    hbm = pl.BlockSpec(memory_space=pltpu.HBM)
    bf16, f32 = jnp.bfloat16, jnp.float32
    return pl.pallas_call(
        kernel,
        out_shape=jax.ShapeDtypeStruct((rows, samples, width), bf16),
        in_specs=[hbm] * 6,
        out_specs=pl.BlockSpec(memory_space=pltpu.VMEM),
        scratch_shapes=[
            pltpu.VMEM((rows, samples, width), bf16),
            pltpu.VMEM((2, rows * PITCH, 128), f32),
            pltpu.VMEM((chunks, group, rows, width), bf16),
            pltpu.VMEM((chunks, emb_count, width), bf16),
            pltpu.VMEM((emb_count + rank, emb_count), bf16),
            pltpu.VMEM((chunks, emb_count, width), bf16),
            pltpu.VMEM((chunks, group, rows, width), bf16),
            pltpu.VMEM((emb_count, width), f32),
            pltpu.VMEM(w_fmb.shape, bf16),
            pltpu.VMEM(ln_gain.shape, f32),
            pltpu.VMEM(ln_bias.shape, f32),
            pltpu.SemaphoreType.DMA((chunks,)),
            pltpu.SemaphoreType.DMA((5,)),
            pltpu.SemaphoreType.DMA((chunks,)),
            pltpu.SemaphoreType.DMA((chunks,)),
            pltpu.SemaphoreType.DMA((chunks,)),
            pltpu.SemaphoreType.DMA((chunks,)),
            pltpu.SemaphoreType.DMA((emb_count // w_lcb.shape[0] - 1,)),
            pltpu.SemaphoreType.DMA,
        ],
        compiler_params=pltpu.CompilerParams(
            collective_id=0, has_side_effects=True, vmem_limit_bytes=67043328
        ),
        name="wukong",
    )(embeddings, machine_projection.T, w_lcb, w_fmb, ln_gain, ln_bias)


def solution(mesh):
    placed = (P("emb", "dp", None), P(), P("dp", None), P(), P("emb", None), P("emb", None))
    return jax.shard_map(
        body, mesh=mesh, in_specs=placed, out_specs=P("emb", "dp", None), check_vma=False
    )
```

```python
import functools

import jax
import jax.numpy as jnp
from jax import lax
from jax.experimental import pallas as pl
from jax.experimental.pallas import tpu as pltpu
from jax.sharding import PartitionSpec as P

MESH = pl.DeviceIdType.MESH
PEERS = ((0, 1),) + tuple((d, c) for d in (1, 7, 2, 6, 3, 5, 4) for c in (0, 1))
PITCH = 24


def kernel(
    emb_ref, mp_ref, w_ref, wf_ref, g_ref, b_ref, out_ref,
    ebuf, stage, sendbuf, xbuf, wfull, rbuf, ybuf, mixed, wf_v, g_v, b_v,
    load_sem, small_sem, in_send, in_recv, out_send, out_recv, w_send, w_recv,
):
    e = lax.axis_index("emb")
    dp = lax.axis_index("dp")
    z, c = e // 2, e % 2
    rows, samples, width = ebuf.shape
    chunks, group = sendbuf.shape[0], sendbuf.shape[1]
    emb_count = xbuf.shape[1]
    y, x = dp % 4, dp // 4
    ring = (x * 4 + (y + 1) % 4, x * 4 + (y + 3) % 4, (x + 1) % 4 * 4 + y, (x + 3) % 4 * 4 + y)

    def peer(d, cc):
        return lax.rem(z + d, 8) * 2 + lax.rem(c + cc, 2)

    barrier = pltpu.get_barrier_semaphore()
    for d, cc in PEERS:
        pl.semaphore_signal(barrier, inc=1, device_id={"emb": peer(d, cc)}, device_id_type=MESH)
    for k in range(4):
        pl.semaphore_signal(barrier, inc=1, device_id={"dp": ring[k]}, device_id_type=MESH)

    def load(s):
        part = pl.ds(s * group, group)
        return pltpu.make_async_copy(emb_ref.at[:, part], ebuf.at[:, part], load_sem.at[s])

    my_w = pl.ds(pl.multiple_of(dp * rows, rows), rows)
    load(0).start()
    own_w = pltpu.make_async_copy(w_ref, wfull.at[my_w], small_sem.at[0])
    own_w.start()
    for s in range(1, chunks):
        load(s).start()
    small = [
        pltpu.make_async_copy(a, v, small_sem.at[1 + i])
        for i, (a, v) in enumerate(((mp_ref, wfull.at[pl.ds(emb_count, mp_ref.shape[0])]), (wf_ref, wf_v), (g_ref, g_v), (b_ref, b_v)))
    ]
    for copy in small:
        copy.start()

    my_rows = pl.ds(pl.multiple_of(e * rows, rows), rows)

    def prepare(s):
        load(s).wait()
        for n in range(rows):
            block = ebuf[n, pl.ds(pl.multiple_of(s * group, group), group), :].astype(jnp.float32)
            for h in range(2):
                stage[h, pl.ds(n * PITCH, group), :] = block[:, h * 128 : (h + 1) * 128]
        for b in range(group):
            for h in range(2):
                sendbuf[s, b, :, pl.ds(h * 128, 128)] = stage[h, pl.ds(b, rows, stride=PITCH), :].astype(jnp.bfloat16)
        xbuf[s, my_rows, :] = sendbuf[s, e]

    def send_in(s):
        for i, (d, cc) in enumerate(PEERS):
            j = peer(d, cc)
            pltpu.make_async_remote_copy(
                src_ref=sendbuf.at[s, j], dst_ref=xbuf.at[s, my_rows],
                send_sem=in_send.at[s], recv_sem=in_recv.at[s],
                device_id={"emb": j}, device_id_type=MESH,
            ).start()

    def w_copy(i, to, start, size):
        part = pl.ds(pl.multiple_of(start, 16), size)
        return pltpu.make_async_remote_copy(
            src_ref=wfull.at[part], dst_ref=wfull.at[part], send_sem=w_send.at[i], recv_sem=w_recv.at[i],
            device_id={"dp": ring[to]}, device_id_type=MESH,
        )

    column = x * 4 * rows
    w_copies = (
        w_copy(0, 0, column + y * rows, rows),
        w_copy(1, 1, column + y * rows, rows),
        w_copy(2, 0, column + (y + 3) % 4 * rows, rows // 2),
        w_copy(3, 1, column + (y + 1) % 4 * rows + rows // 2, rows // 2),
        w_copy(4, 2, column, 4 * rows),
        w_copy(5, 3, column, 4 * rows),
        w_copy(6, 2, (x + 3) % 4 * 4 * rows, 2 * rows),
        w_copy(7, 3, (x + 1) % 4 * 4 * rows + 2 * rows, 2 * rows),
    )

    prepare(0)
    own_w.wait()
    pl.semaphore_wait(barrier, len(PEERS) + 4)
    send_in(0)
    w_copies[0].start()
    w_copies[1].start()

    def feed(s, carry):
        prepare(s)
        send_in(s)
        return carry

    lax.fori_loop(1, chunks, feed, 0)

    for first in (0, 2, 4, 6):
        w_copies[first].wait_recv()
        w_copies[first + 1].wait_recv()
        if first < 6:
            w_copies[first + 2].start()
            w_copies[first + 3].start()
    for copy in small:
        copy.wait()
    others = pl.ds(0, emb_count - rows)

    block = 128
    entries = jnp.float32(emb_count * width)

    def mix(s, carry):
        pltpu.make_async_copy(xbuf.at[s, others], xbuf.at[s, others], in_recv.at[s]).wait()
        x = xbuf[s]
        factor = jnp.dot(wfull[pl.ds(emb_count, 32), :], x, preferred_element_type=jnp.float32).astype(jnp.bfloat16)
        total = jnp.zeros((8, width), jnp.float32)
        for i in range(emb_count // block):
            part = pl.ds(i * block, block)
            xb = xbuf[s, part, :]
            inner = lax.dot_general(xb, factor, (((1,), (1,)), ((), ())), preferred_element_type=jnp.float32).astype(jnp.bfloat16)
            m = jnp.dot(wfull[part, :], x, preferred_element_type=jnp.float32)
            m = m + xb.astype(jnp.float32) + jnp.dot(inner, wf_v[...], preferred_element_type=jnp.float32)
            mixed[part, :] = m
            total = total + jnp.sum(m.reshape(block // 8, 8, width), axis=0)
        average = jnp.sum(total, keepdims=True) / entries
        square = jnp.zeros((8, width), jnp.float32)
        for i in range(emb_count // block):
            centered = mixed[pl.ds(i * block, block), :] - average
            square = square + jnp.sum((centered * centered).reshape(block // 8, 8, width), axis=0)
        scale = lax.rsqrt(jnp.sum(square, keepdims=True) / entries + 1e-05)
        for i in range(emb_count // block):
            part = pl.ds(i * block, block)
            rbuf[s, part, :] = ((mixed[part, :] - average) * scale).astype(jnp.bfloat16)
        ybuf[s, e] = rbuf[s, my_rows, :]
        for i, (d, cc) in enumerate(PEERS):
            j = peer(d, cc)
            pltpu.make_async_remote_copy(
                src_ref=rbuf.at[s, pl.ds(pl.multiple_of(j * rows, rows), rows)], dst_ref=ybuf.at[s, e],
                send_sem=out_send.at[s], recv_sem=out_recv.at[s],
                device_id={"emb": j}, device_id_type=MESH,
            ).start()
        return carry

    lax.fori_loop(0, chunks, mix, 0)

    fifteen = pl.ds(0, group - 1)

    def finish(s, carry):
        pltpu.make_async_copy(ybuf.at[s, fifteen], ybuf.at[s, fifteen], out_recv.at[s]).wait()
        part = pl.ds(pl.multiple_of(s * group, group), group)
        for b in range(group):
            y = ybuf[s, b].astype(jnp.float32) * g_v[...] + b_v[...]
            for h in range(2):
                stage[h, pl.ds(b, rows, stride=PITCH), :] = y[:, h * 128 : (h + 1) * 128]
        for n in range(rows):
            for h in range(2):
                out_ref[n, part, pl.ds(h * 128, 128)] = stage[h, pl.ds(n * PITCH, group), :].astype(jnp.bfloat16)
        return carry

    lax.fori_loop(0, chunks, finish, 0)

    def drain(s, carry):
        pltpu.make_async_copy(sendbuf.at[s, fifteen], sendbuf.at[s, fifteen], in_send.at[s]).wait()
        pltpu.make_async_copy(ybuf.at[s, fifteen], ybuf.at[s, fifteen], out_send.at[s]).wait()
        return carry

    lax.fori_loop(0, chunks, drain, 0)
    for copy in w_copies:
        copy.wait_send()


def body(embeddings, machine_projection, w_lcb, w_fmb, ln_gain, ln_bias):
    rows, samples, width = embeddings.shape
    emb_count, rank = machine_projection.shape
    group = emb_count // rows
    chunks = samples // group
    hbm = pl.BlockSpec(memory_space=pltpu.HBM)
    operands = (embeddings, machine_projection.T, w_lcb, w_fmb, ln_gain, ln_bias)
    bf16, f32 = jnp.bfloat16, jnp.float32
    return pl.pallas_call(
        kernel,
        out_shape=pltpu.VMEM((rows, samples, width), bf16),
        in_specs=[hbm] * 6,
        out_specs=pl.BlockSpec(memory_space=pltpu.VMEM),
        scratch_shapes=[
            pltpu.VMEM((rows, samples, width), bf16),
            pltpu.VMEM((2, rows * PITCH, 128), f32),
            pltpu.VMEM((chunks, group, rows, width), bf16),
            pltpu.VMEM((chunks, emb_count, width), bf16),
            pltpu.VMEM((emb_count + rank, emb_count), bf16),
            pltpu.VMEM((chunks, emb_count, width), bf16),
            pltpu.VMEM((chunks, group, rows, width), bf16),
            pltpu.VMEM((emb_count, width), f32),
            pltpu.VMEM(w_fmb.shape, bf16),
            pltpu.VMEM(ln_gain.shape, f32),
            pltpu.VMEM(ln_bias.shape, f32),
            pltpu.SemaphoreType.DMA((chunks,)),
            pltpu.SemaphoreType.DMA((5,)),
            pltpu.SemaphoreType.DMA((chunks,)),
            pltpu.SemaphoreType.DMA((chunks,)),
            pltpu.SemaphoreType.DMA((chunks,)),
            pltpu.SemaphoreType.DMA((chunks,)),
            pltpu.SemaphoreType.DMA((8,)),
            pltpu.SemaphoreType.DMA((8,)),
        ],
        compiler_params=pltpu.CompilerParams(
            collective_id=0, has_side_effects=True, vmem_limit_bytes=48 << 20
        ),
        name="wukong",
    )(*(pltpu.with_memory_space_constraint(a, pltpu.HBM) for a in operands))


def solution(mesh):
    placed = (P("emb", "dp", None), P(), P("dp", None), P(), P("emb", None), P("emb", None))
    return jax.shard_map(
        body, mesh=mesh, in_specs=placed, out_specs=P("emb", "dp", None), check_vma=False
    )
```

```python
import functools

import jax
import jax.numpy as jnp
from jax import lax
from jax.experimental import pallas as pl
from jax.experimental.pallas import tpu as pltpu
from jax.sharding import PartitionSpec as P

MESH = pl.DeviceIdType.MESH
PEERS = ((0, 1),) + tuple((d, c) for d in (1, 7, 2, 6, 3, 5, 4) for c in (0, 1))
PITCH = 24


def kernel(
    emb_ref, mp_ref, w_ref, wf_ref, g_ref, b_ref, out_ref,
    ebuf, stage, sendbuf, xbuf, wfull, rbuf, ybuf, mixed, wf_v, g_v, b_v,
    load_sem, small_sem, in_send, in_recv, out_send, out_recv, w_send, w_recv, ready, dp_ready, told,
):
    e = lax.axis_index("emb")
    dp = lax.axis_index("dp")
    z, c = e // 2, e % 2
    rows, samples, width = ebuf.shape
    chunks, group = sendbuf.shape[0], sendbuf.shape[1]
    emb_count = xbuf.shape[1]
    y, x = dp % 4, dp // 4
    ring = (x * 4 + (y + 1) % 4, x * 4 + (y + 3) % 4, (x + 1) % 4 * 4 + y, (x + 3) % 4 * 4 + y)

    def peer(d, cc):
        return lax.rem(z + d, 8) * 2 + lax.rem(c + cc, 2)

    def first(d, cc):
        return c == jnp.minimum(z, 1) if d == 0 else peer(d, cc) // 2 < z

    def signal(semaphore, device):
        pl.semaphore_signal(semaphore, inc=1, device_id=device, device_id_type=MESH)

    half = 4
    late = z >= half

    def apart(d, cc):
        return jnp.logical_and(late, peer(d, cc) >= 2 * half) if d in (2, 3, 5, 6) else False

    barrier = pltpu.get_barrier_semaphore()
    heard = 2 * jnp.where(late, half + jnp.minimum(z - half, 1), z) + (c == jnp.minimum(z, 1)).astype(jnp.int32)
    for d, cc in PEERS:
        pl.when(jnp.logical_not(jnp.logical_or(first(d, cc), apart(d, cc))))(functools.partial(signal, barrier, {"emb": peer(d, cc)}))
    answers = 0
    for k in range(4):
        pl.when(ring[k] > dp)(functools.partial(signal, barrier, {"dp": ring[k]}))
        heard = heard + (ring[k] < dp).astype(jnp.int32)
        answers = answers + (ring[k] > dp).astype(jnp.int32)

    def load(s):
        part = pl.ds(s * group, group)
        return pltpu.make_async_copy(emb_ref.at[:, part], ebuf.at[:, part], load_sem.at[s])

    my_w = pl.ds(pl.multiple_of(dp * rows, rows), rows)
    load(0).start()
    my_half = pl.ds(pl.multiple_of(c * (emb_count // 2), 128), emb_count // 2)
    own_w = pltpu.make_async_copy(w_ref.at[:, my_half], wfull.at[my_w, my_half], small_sem.at[0])
    own_w.start()
    for s in range(1, chunks):
        load(s).start()
    small = [
        pltpu.make_async_copy(a, v, small_sem.at[1 + i])
        for i, (a, v) in enumerate(((mp_ref, wfull.at[pl.ds(emb_count, mp_ref.shape[0])]), (wf_ref, wf_v), (g_ref, g_v), (b_ref, b_v)))
    ]
    for copy in small:
        copy.start()

    pl.when(heard > 0)(lambda: pl.semaphore_wait(barrier, heard))
    for d, cc in PEERS:
        pl.when(jnp.logical_and(first(d, cc), jnp.logical_not(apart(d, cc))))(functools.partial(signal, ready.at[e], {"emb": peer(d, cc)}))
    for k in range(4):
        pl.when(ring[k] < dp)(functools.partial(signal, dp_ready, {"dp": ring[k]}))

    my_rows = pl.ds(pl.multiple_of(e * rows, rows), rows)

    def prepare(s):
        load(s).wait()
        for n in range(rows):
            block = ebuf[n, pl.ds(pl.multiple_of(s * group, group), group), :].astype(jnp.float32)
            for h in range(2):
                stage[h, pl.ds(n * PITCH, group), :] = block[:, h * 128 : (h + 1) * 128]
        for b in range(group):
            for h in range(2):
                sendbuf[s, b, :, pl.ds(h * 128, 128)] = stage[h, pl.ds(b, rows, stride=PITCH), :].astype(jnp.bfloat16)
        xbuf[s, my_rows, :] = sendbuf[s, e]

    def send_one(s, j):
        pltpu.make_async_remote_copy(
            src_ref=sendbuf.at[s, j], dst_ref=xbuf.at[s, my_rows],
            send_sem=in_send.at[s], recv_sem=in_recv.at[s],
            device_id={"emb": j}, device_id_type=MESH,
        ).start()

    def send_to(s, to_late, to_early):
        for d, cc in PEERS:
            if to_late and to_early:
                send_one(s, peer(d, cc))
            else:
                pl.when((peer(d, cc) >= 2 * half) == to_late)(functools.partial(send_one, s, peer(d, cc)))

    def await_peer(d, cc):
        pl.when(jnp.logical_not(first(d, cc)))(lambda: pl.semaphore_wait(ready.at[peer(d, cc)], 1))

    def w_copy(i, to, start, size):
        part = pl.ds(pl.multiple_of(start, 16), size)
        return pltpu.make_async_remote_copy(
            src_ref=wfull.at[part, my_half], dst_ref=wfull.at[part, my_half], send_sem=w_send.at[i], recv_sem=w_recv.at[i],
            device_id={"dp": ring[to]}, device_id_type=MESH,
        )

    column = x * 4 * rows
    w_copies = (
        w_copy(0, 0, column + y * rows, rows),
        w_copy(1, 1, column + y * rows, rows),
        w_copy(2, 0, column + (y + 3) % 4 * rows, rows // 2),
        w_copy(3, 1, column + (y + 1) % 4 * rows + rows // 2, rows // 2),
        w_copy(4, 2, column, 4 * rows),
        w_copy(5, 3, column, 4 * rows),
        w_copy(6, 2, (x + 3) % 4 * 4 * rows, 2 * rows),
        w_copy(7, 3, (x + 1) % 4 * 4 * rows + 2 * rows, 2 * rows),
    )

    def start_weights():
        own_w.wait()
        pl.when(answers > 0)(lambda: pl.semaphore_wait(dp_ready, answers))
        w_copies[0].start()
        w_copies[1].start()

    @pl.when(jnp.logical_not(late))
    def _():
        def ready_made(s, carry):
            prepare(s)
            return carry

        lax.fori_loop(0, chunks, ready_made, 0)
        for d, cc in PEERS:

            @pl.when(peer(d, cc) < 2 * half)
            def _(d=d, cc=cc):
                await_peer(d, cc)
                for s in range(4):
                    send_one(s, peer(d, cc))

        start_weights()
        for d, cc in PEERS:

            @pl.when(peer(d, cc) >= 2 * half)
            def _(d=d, cc=cc):
                await_peer(d, cc)
                send_one(0, peer(d, cc))

        send_to(1, True, False)
        send_to(2, True, False)
        send_to(3, True, False)

    @pl.when(late)
    def _():
        for s in range(2):
            prepare(s)
            send_to(s, False, True)
        for s in range(2, 4):
            prepare(s)

        def tell(d, about):
            signal(told.at[about], {"emb": peer(d, 0)})

        for d, cc in PEERS[:5]:

            @pl.when(peer(d, cc) >= 2 * half)
            def _(d=d, cc=cc):
                await_peer(d, cc)
                send_one(0, peer(d, cc))

        @pl.when(jnp.logical_and(z > half, z < 7))
        def _():
            tell(1, z - 1)
            tell(7, z + 1)

        start_weights()
        for d in (6, 2, 5, 3):
            about = lax.rem(z + d, 8)

            @pl.when(apart(d, 0))
            def _(d=d, about=about):
                pl.semaphore_wait(told.at[about], 1)
                if d == 6:
                    pl.when(z == half + 2)(lambda: tell(1, about))
                if d == 2:
                    pl.when(z == half + 1)(lambda: tell(7, about))
                for cc in range(2):
                    send_one(0, peer(d, cc))

        send_to(1, True, False)
        send_to(2, True, True)
        send_to(3, True, True)

    for i in (0, 2, 4, 6):
        w_copies[i].wait_recv()
        w_copies[i + 1].wait_recv()
        if i < 6:
            w_copies[i + 2].start()
            w_copies[i + 3].start()
    whole = pl.ds(0, emb_count)
    swap = pltpu.make_async_remote_copy(
        src_ref=wfull.at[whole, my_half], dst_ref=wfull.at[whole, my_half], send_sem=w_send.at[8], recv_sem=w_recv.at[8],
        device_id={"emb": peer(0, 1)}, device_id_type=MESH,
    )
    swap.start()
    for copy in small:
        copy.wait()
    swap.wait_recv()
    others = pl.ds(0, emb_count - rows)

    block = 128
    entries = jnp.float32(emb_count * width)

    def out_one(s, j):
        pltpu.make_async_remote_copy(
            src_ref=rbuf.at[s, pl.ds(pl.multiple_of(j * rows, rows), rows)], dst_ref=ybuf.at[s, e],
            send_sem=out_send.at[s], recv_sem=out_recv.at[s],
            device_id={"emb": j}, device_id_type=MESH,
        ).start()

    def send_out(s):
        def relative():
            for d, cc in PEERS:
                out_one(s, peer(d, cc))

        def absolute():
            for j in range(16):
                pl.when(j != e)(functools.partial(out_one, s, j))

        pl.when(s < 2)(relative)
        pl.when(s >= 2)(absolute)

    def mix(s, carry):
        pltpu.make_async_copy(xbuf.at[s, others], xbuf.at[s, others], in_recv.at[s]).wait()
        x = xbuf[s]
        factor = jnp.dot(wfull[pl.ds(emb_count, 32), :], x, preferred_element_type=jnp.float32).astype(jnp.bfloat16)
        total = jnp.zeros((8, width), jnp.float32)
        for i in range(emb_count // block):
            part = pl.ds(i * block, block)
            xb = xbuf[s, part, :]
            inner = lax.dot_general(xb, factor, (((1,), (1,)), ((), ())), preferred_element_type=jnp.float32).astype(jnp.bfloat16)
            m = jnp.dot(wfull[part, :], x, preferred_element_type=jnp.float32)
            m = m + xb.astype(jnp.float32) + jnp.dot(inner, wf_v[...], preferred_element_type=jnp.float32)
            mixed[part, :] = m
            total = total + jnp.sum(m.reshape(block // 8, 8, width), axis=0)
        average = jnp.sum(total, keepdims=True) / entries
        square = jnp.zeros((8, width), jnp.float32)
        for i in range(emb_count // block):
            centered = mixed[pl.ds(i * block, block), :] - average
            square = square + jnp.sum((centered * centered).reshape(block // 8, 8, width), axis=0)
        scale = lax.rsqrt(jnp.sum(square, keepdims=True) / entries + 1e-05)
        for i in range(emb_count // block):
            part = pl.ds(i * block, block)
            rbuf[s, part, :] = ((mixed[part, :] - average) * scale).astype(jnp.bfloat16)
        ybuf[s, e] = rbuf[s, my_rows, :]
        send_out(s)
        return carry

    lax.fori_loop(0, chunks, mix, 0)

    fifteen = pl.ds(0, group - 1)

    def finish(s, carry):
        pltpu.make_async_copy(ybuf.at[s, fifteen], ybuf.at[s, fifteen], out_recv.at[s]).wait()
        part = pl.ds(pl.multiple_of(s * group, group), group)
        for b in range(group):
            y = ybuf[s, b].astype(jnp.float32) * g_v[...] + b_v[...]
            for h in range(2):
                stage[h, pl.ds(b, rows, stride=PITCH), :] = y[:, h * 128 : (h + 1) * 128]
        for n in range(rows):
            for h in range(2):
                out_ref[n, part, pl.ds(h * 128, 128)] = stage[h, pl.ds(n * PITCH, group), :].astype(jnp.bfloat16)
        return carry

    lax.fori_loop(0, chunks, finish, 0)

    def drain(s, carry):
        pltpu.make_async_copy(sendbuf.at[s, fifteen], sendbuf.at[s, fifteen], in_send.at[s]).wait()
        pltpu.make_async_copy(ybuf.at[s, fifteen], ybuf.at[s, fifteen], out_send.at[s]).wait()
        return carry

    lax.fori_loop(0, chunks, drain, 0)
    for copy in w_copies:
        copy.wait_send()
    swap.wait_send()


def body(embeddings, machine_projection, w_lcb, w_fmb, ln_gain, ln_bias):
    rows, samples, width = embeddings.shape
    emb_count, rank = machine_projection.shape
    group = emb_count // rows
    chunks = samples // group
    hbm = pl.BlockSpec(memory_space=pltpu.HBM)
    operands = (embeddings, machine_projection.T, w_lcb, w_fmb, ln_gain, ln_bias)
    bf16, f32 = jnp.bfloat16, jnp.float32
    return pl.pallas_call(
        kernel,
        out_shape=pltpu.VMEM((rows, samples, width), bf16),
        in_specs=[hbm] * 6,
        out_specs=pl.BlockSpec(memory_space=pltpu.VMEM),
        scratch_shapes=[
            pltpu.VMEM((rows, samples, width), bf16),
            pltpu.VMEM((2, rows * PITCH, 128), f32),
            pltpu.VMEM((chunks, group, rows, width), bf16),
            pltpu.VMEM((chunks, emb_count, width), bf16),
            pltpu.VMEM((emb_count + rank, emb_count), bf16),
            pltpu.VMEM((chunks, emb_count, width), bf16),
            pltpu.VMEM((chunks, group, rows, width), bf16),
            pltpu.VMEM((emb_count, width), f32),
            pltpu.VMEM(w_fmb.shape, bf16),
            pltpu.VMEM(ln_gain.shape, f32),
            pltpu.VMEM(ln_bias.shape, f32),
            pltpu.SemaphoreType.DMA((chunks,)),
            pltpu.SemaphoreType.DMA((5,)),
            pltpu.SemaphoreType.DMA((chunks,)),
            pltpu.SemaphoreType.DMA((chunks,)),
            pltpu.SemaphoreType.DMA((chunks,)),
            pltpu.SemaphoreType.DMA((chunks,)),
            pltpu.SemaphoreType.DMA((9,)),
            pltpu.SemaphoreType.DMA((9,)),
            pltpu.SemaphoreType.REGULAR((group,)),
            pltpu.SemaphoreType.REGULAR,
            pltpu.SemaphoreType.REGULAR((8,)),
        ],
        compiler_params=pltpu.CompilerParams(
            collective_id=0, has_side_effects=True, vmem_limit_bytes=48 << 20
        ),
        name="wukong",
    )(*(pltpu.with_memory_space_constraint(a, pltpu.HBM) for a in operands))


def solution(mesh):
    placed = (P("emb", "dp", None), P(), P("dp", None), P(), P("emb", None), P("emb", None))
    return jax.shard_map(
        body, mesh=mesh, in_specs=placed, out_specs=P("emb", "dp", None), check_vma=False
    )
```

```python
import functools

import jax
import jax.numpy as jnp
from jax import lax
from jax.experimental import pallas as pl
from jax.experimental.pallas import tpu as pltpu
from jax.sharding import PartitionSpec as P

MESH = pl.DeviceIdType.MESH
PEERS = ((0, 1),) + tuple((d, c) for d in (1, 7, 2, 6, 3, 5, 4) for c in (0, 1))
PITCH = 24


def kernel(
    emb_ref, mp_ref, w_ref, wf_ref, g_ref, b_ref, out_ref,
    ebuf, stage, sendbuf, xbuf, wfull, rbuf, ybuf, mixed, wf_v, g_v, b_v,
    load_sem, small_sem, in_send, in_recv, out_send, out_recv, w_send, w_recv, ready, dp_ready, told,
):
    e = lax.axis_index("emb")
    dp = lax.axis_index("dp")
    z, c = e // 2, e % 2
    rows, samples, width = ebuf.shape
    chunks, group = sendbuf.shape[0], sendbuf.shape[1]
    emb_count = xbuf.shape[1]
    y, x = dp % 4, dp // 4
    ring = (x * 4 + (y + 1) % 4, x * 4 + (y + 3) % 4, (x + 1) % 4 * 4 + y, (x + 3) % 4 * 4 + y)

    def peer(d, cc):
        return lax.rem(z + d, 8) * 2 + lax.rem(c + cc, 2)

    def load(s):
        part = pl.ds(s * group, group)
        return pltpu.make_async_copy(emb_ref.at[:, part], ebuf.at[:, part], load_sem.at[s])

    load(0).start()

    def place(chip):
        return jnp.where(chip == 7, 11, 2 * chip)

    def first(d, cc):
        return c == jnp.minimum(z, 1) if d == 0 else place(peer(d, cc) // 2) < place(z)

    def signal(semaphore, device):
        pl.semaphore_signal(semaphore, inc=1, device_id=device, device_id_type=MESH)

    half = 4
    late = z >= half

    def apart(d, cc):
        return jnp.logical_and(late, peer(d, cc) >= 2 * half) if d in (2, 3, 5, 6) else False

    barrier = pltpu.get_barrier_semaphore()
    heard = 2 * jnp.where(late, half + jnp.where(z == half + 1, 1, jnp.where(z == half + 2, 2, 0)), z) + (c == jnp.minimum(z, 1)).astype(jnp.int32)
    for d, cc in PEERS:
        pl.when(jnp.logical_not(jnp.logical_or(first(d, cc), apart(d, cc))))(functools.partial(signal, barrier, {"emb": peer(d, cc)}))
    answers = 0
    for k in range(4):
        pl.when(ring[k] > dp)(functools.partial(signal, barrier, {"dp": ring[k]}))
        heard = heard + (ring[k] < dp).astype(jnp.int32)
        answers = answers + (ring[k] > dp).astype(jnp.int32)

    my_w = pl.ds(pl.multiple_of(dp * rows, rows), rows)
    my_half = pl.ds(pl.multiple_of(c * (emb_count // 2), 128), emb_count // 2)
    own_w = pltpu.make_async_copy(w_ref.at[:, my_half], wfull.at[my_w, my_half], small_sem.at[0])
    own_w.start()
    for s in range(1, chunks):
        load(s).start()
    small = [
        pltpu.make_async_copy(a, v, small_sem.at[1 + i])
        for i, (a, v) in enumerate(((mp_ref, wfull.at[pl.ds(emb_count, mp_ref.shape[0])]), (wf_ref, wf_v), (g_ref, g_v), (b_ref, b_v)))
    ]
    for copy in small:
        copy.start()

    pl.when(heard > 0)(lambda: pl.semaphore_wait(barrier, heard))
    for d, cc in PEERS:
        pl.when(jnp.logical_and(first(d, cc), jnp.logical_not(apart(d, cc))))(functools.partial(signal, ready.at[e], {"emb": peer(d, cc)}))
    for k in range(4):
        pl.when(ring[k] < dp)(functools.partial(signal, dp_ready, {"dp": ring[k]}))

    my_rows = pl.ds(pl.multiple_of(e * rows, rows), rows)

    def prepare(s):
        load(s).wait()
        for n in range(rows):
            block = ebuf[n, pl.ds(pl.multiple_of(s * group, group), group), :].astype(jnp.float32)
            for h in range(2):
                stage[h, pl.ds(n * PITCH, group), :] = block[:, h * 128 : (h + 1) * 128]
        for b in range(group):
            for h in range(2):
                sendbuf[s, b, :, pl.ds(h * 128, 128)] = stage[h, pl.ds(b, rows, stride=PITCH), :].astype(jnp.bfloat16)
        xbuf[s, my_rows, :] = sendbuf[s, e]

    def send_one(s, j):
        pltpu.make_async_remote_copy(
            src_ref=sendbuf.at[s, j], dst_ref=xbuf.at[s, my_rows],
            send_sem=in_send, recv_sem=in_recv.at[s],
            device_id={"emb": j}, device_id_type=MESH,
        ).start()

    def send_to(s, to_late, to_early):
        for d, cc in PEERS:
            if to_late and to_early:
                send_one(s, peer(d, cc))
            else:
                pl.when((peer(d, cc) >= 2 * half) == to_late)(functools.partial(send_one, s, peer(d, cc)))

    def await_peer(d, cc):
        pl.when(jnp.logical_not(first(d, cc)))(lambda: pl.semaphore_wait(ready.at[peer(d, cc)], 1))

    def w_copy(i, to, start, size):
        part = pl.ds(pl.multiple_of(start, 16), size)
        return pltpu.make_async_remote_copy(
            src_ref=wfull.at[part, my_half], dst_ref=wfull.at[part, my_half], send_sem=w_send, recv_sem=w_recv.at[i],
            device_id={"dp": ring[to]}, device_id_type=MESH,
        )

    column = x * 4 * rows
    w_copies = (
        w_copy(0, 0, column + y * rows, rows),
        w_copy(1, 1, column + y * rows, rows),
        w_copy(2, 0, column + (y + 3) % 4 * rows, rows // 2),
        w_copy(3, 1, column + (y + 1) % 4 * rows + rows // 2, rows // 2),
        w_copy(4, 2, column, 4 * rows),
        w_copy(5, 3, column, 4 * rows),
        w_copy(6, 2, (x + 3) % 4 * 4 * rows, 2 * rows),
        w_copy(7, 3, (x + 1) % 4 * 4 * rows + 2 * rows, 2 * rows),
    )

    def start_weights():
        own_w.wait()
        pl.when(answers > 0)(lambda: pl.semaphore_wait(dp_ready, answers))
        w_copies[0].start()
        w_copies[1].start()

    @pl.when(jnp.logical_not(late))
    def _():
        def ready_made(s, carry):
            prepare(s)
            return carry

        lax.fori_loop(0, chunks, ready_made, 0)
        for d, cc in PEERS:

            @pl.when(peer(d, cc) < 2 * half)
            def _(d=d, cc=cc):
                await_peer(d, cc)
                for s in range(4):
                    send_one(s, peer(d, cc))

        start_weights()
        for d, cc in PEERS:

            @pl.when(peer(d, cc) >= 2 * half)
            def _(d=d, cc=cc):
                await_peer(d, cc)
                send_one(0, peer(d, cc))

        send_to(1, True, False)
        send_to(2, True, False)
        send_to(3, True, False)

    @pl.when(late)
    def _():
        for s in range(2):
            prepare(s)
            send_to(s, False, True)
        for s in range(2, 4):
            prepare(s)

        def tell(d, about):
            signal(told.at[about - half], {"emb": peer(d, 0)})

        for d, cc in PEERS[:5]:

            @pl.when(peer(d, cc) >= 2 * half)
            def _(d=d, cc=cc):
                await_peer(d, cc)
                send_one(0, peer(d, cc))

        @pl.when(jnp.logical_and(z > half, z < 7))
        def _():
            tell(1, z - 1)
            tell(7, z + 1)

        start_weights()
        for d in (6, 2, 5, 3):
            about = lax.rem(z + d, 8)

            @pl.when(apart(d, 0))
            def _(d=d, about=about):
                pl.semaphore_wait(told.at[about - half], 1)
                if d == 6:
                    pl.when(z == half + 2)(lambda: tell(1, about))
                if d == 2:
                    pl.when(z == half + 1)(lambda: tell(7, about))
                for cc in range(2):
                    send_one(0, peer(d, cc))

        send_to(1, True, False)
        send_to(2, True, True)
        send_to(3, True, True)

    for i in (0, 2, 4, 6):
        w_copies[i].wait_recv()
        w_copies[i + 1].wait_recv()
        if i < 6:
            w_copies[i + 2].start()
            w_copies[i + 3].start()
    whole = pl.ds(0, emb_count)
    swap = pltpu.make_async_remote_copy(
        src_ref=wfull.at[whole, my_half], dst_ref=wfull.at[whole, my_half], send_sem=w_send, recv_sem=w_recv.at[8],
        device_id={"emb": peer(0, 1)}, device_id_type=MESH,
    )
    swap.start()
    for copy in small:
        copy.wait()
    swap.wait_recv()
    others = pl.ds(0, emb_count - rows)

    block = 128
    entries = jnp.float32(emb_count * width)

    def out_one(s, j):
        pltpu.make_async_remote_copy(
            src_ref=rbuf.at[s, pl.ds(pl.multiple_of(j * rows, rows), rows)], dst_ref=ybuf.at[s, e],
            send_sem=out_send, recv_sem=out_recv.at[s],
            device_id={"emb": j}, device_id_type=MESH,
        ).start()

    def send_out(s):
        def relative():
            for d, cc in PEERS:
                out_one(s, peer(d, cc))

        def absolute():
            for j in range(16):
                pl.when(j != e)(functools.partial(out_one, s, j))

        def across(nearest):
            if nearest:
                for d, cc in PEERS:
                    pl.when((peer(d, cc) >= 2 * half) != late)(functools.partial(out_one, s, peer(d, cc)))
            else:
                for j in range(2 * half):
                    pl.when(late)(functools.partial(out_one, s, j))
                for d, cc in PEERS:
                    pl.when(jnp.logical_and(peer(d, cc) >= 2 * half, jnp.logical_not(late)))(functools.partial(out_one, s, peer(d, cc)))
            for j in range(4 * half):
                pl.when(jnp.logical_and(j != e, (j >= 2 * half) == late))(functools.partial(out_one, s, j))

        pl.when(s < 2)(relative)
        pl.when(s >= 2)(absolute)

    def mix(s, carry):
        pltpu.make_async_copy(xbuf.at[s, others], xbuf.at[s, others], in_recv.at[s]).wait()
        x = xbuf[s]
        factor = jnp.dot(wfull[pl.ds(emb_count, 32), :], x, preferred_element_type=jnp.float32).astype(jnp.bfloat16)
        total = jnp.zeros((8, width), jnp.float32)
        for i in range(emb_count // block):
            part = pl.ds(i * block, block)
            xb = xbuf[s, part, :]
            inner = lax.dot_general(xb, factor, (((1,), (1,)), ((), ())), preferred_element_type=jnp.float32).astype(jnp.bfloat16)
            m = jnp.dot(wfull[part, :], x, preferred_element_type=jnp.float32)
            m = m + xb.astype(jnp.float32) + jnp.dot(inner, wf_v[...], preferred_element_type=jnp.float32)
            mixed[part, :] = m
            total = total + jnp.sum(m.reshape(block // 8, 8, width), axis=0)
        average = jnp.sum(total, keepdims=True) / entries
        square = jnp.zeros((8, width), jnp.float32)
        for i in range(emb_count // block):
            centered = mixed[pl.ds(i * block, block), :] - average
            square = square + jnp.sum((centered * centered).reshape(block // 8, 8, width), axis=0)
        scale = lax.rsqrt(jnp.sum(square, keepdims=True) / entries + 1e-05)
        for i in range(emb_count // block):
            part = pl.ds(i * block, block)
            rbuf[s, part, :] = ((mixed[part, :] - average) * scale).astype(jnp.bfloat16)
        ybuf[s, e] = rbuf[s, my_rows, :]
        send_out(s)
        return carry

    lax.fori_loop(0, chunks, mix, 0)

    fifteen = pl.ds(0, group - 1)

    def finish(s, carry):
        pltpu.make_async_copy(ybuf.at[s, fifteen], ybuf.at[s, fifteen], out_recv.at[s]).wait()
        part = pl.ds(pl.multiple_of(s * group, group), group)
        for b in range(group):
            y = ybuf[s, b].astype(jnp.float32) * g_v[...] + b_v[...]
            for h in range(2):
                stage[h, pl.ds(b, rows, stride=PITCH), :] = y[:, h * 128 : (h + 1) * 128]
        for n in range(rows):
            for h in range(2):
                out_ref[n, part, pl.ds(h * 128, 128)] = stage[h, pl.ds(n * PITCH, group), :].astype(jnp.bfloat16)
        return carry

    lax.fori_loop(0, chunks, finish, 0)

    sent = pltpu.make_async_copy(sendbuf.at[:, fifteen], sendbuf.at[:, fifteen], in_send)
    sent.wait()
    sent = pltpu.make_async_copy(ybuf.at[:, fifteen], ybuf.at[:, fifteen], out_send)
    sent.wait()
    passed = pl.ds(0, emb_count - rows // 2)
    pltpu.make_async_copy(wfull.at[passed], wfull.at[passed], w_send).wait()


def body(embeddings, machine_projection, w_lcb, w_fmb, ln_gain, ln_bias):
    rows, samples, width = embeddings.shape
    emb_count, rank = machine_projection.shape
    group = emb_count // rows
    chunks = samples // group
    hbm = pl.BlockSpec(memory_space=pltpu.HBM)
    operands = (embeddings, machine_projection.T, w_lcb, w_fmb, ln_gain, ln_bias)
    bf16, f32 = jnp.bfloat16, jnp.float32
    return pl.pallas_call(
        kernel,
        out_shape=pltpu.VMEM((rows, samples, width), bf16),
        in_specs=[hbm] * 6,
        out_specs=pl.BlockSpec(memory_space=pltpu.VMEM),
        scratch_shapes=[
            pltpu.VMEM((rows, samples, width), bf16),
            pltpu.VMEM((2, rows * PITCH, 128), f32),
            pltpu.VMEM((chunks, group, rows, width), bf16),
            pltpu.VMEM((chunks, emb_count, width), bf16),
            pltpu.VMEM((emb_count + rank, emb_count), bf16),
            pltpu.VMEM((chunks, emb_count, width), bf16),
            pltpu.VMEM((chunks, group, rows, width), bf16),
            pltpu.VMEM((emb_count, width), f32),
            pltpu.VMEM(w_fmb.shape, bf16),
            pltpu.VMEM(ln_gain.shape, f32),
            pltpu.VMEM(ln_bias.shape, f32),
            pltpu.SemaphoreType.DMA((chunks,)),
            pltpu.SemaphoreType.DMA((5,)),
            pltpu.SemaphoreType.DMA,
            pltpu.SemaphoreType.DMA((chunks,)),
            pltpu.SemaphoreType.DMA,
            pltpu.SemaphoreType.DMA((chunks,)),
            pltpu.SemaphoreType.DMA,
            pltpu.SemaphoreType.DMA((9,)),
            pltpu.SemaphoreType.REGULAR((group,)),
            pltpu.SemaphoreType.REGULAR,
            pltpu.SemaphoreType.REGULAR((4,)),
        ],
        compiler_params=pltpu.CompilerParams(
            collective_id=0, has_side_effects=True, vmem_limit_bytes=48 << 20
        ),
        name="wukong",
    )(*(pltpu.with_memory_space_constraint(a, pltpu.HBM) for a in operands))


def solution(mesh):
    placed = (P("emb", "dp", None), P(), P("dp", None), P(), P("emb", None), P("emb", None))
    return jax.shard_map(
        body, mesh=mesh, in_specs=placed, out_specs=P("emb", "dp", None), check_vma=False
    )
```

```python
import functools

import jax
import jax.numpy as jnp
from jax import lax
from jax.experimental import pallas as pl
from jax.experimental.pallas import tpu as pltpu
from jax.sharding import PartitionSpec as P

MESH = pl.DeviceIdType.MESH
PEERS = ((0, 1),) + tuple((d, c) for d in (1, 7, 2, 6, 3, 5, 4) for c in (0, 1))
PITCH = 24


def kernel(
    emb_ref, mp_ref, w_ref, wf_ref, g_ref, b_ref, out_ref,
    ebuf, stage, sendbuf, xbuf, wfull, rbuf, ybuf, mixed, wf_v, g_v, b_v,
    load_sem, small_sem, in_send, in_recv, out_send, out_recv, w_send, w_recv, ready, dp_ready, told,
):
    e = lax.axis_index("emb")
    dp = lax.axis_index("dp")
    z, c = e // 2, e % 2
    rows, samples, width = ebuf.shape
    rank = mp_ref.shape[0]
    chunks, group = sendbuf.shape[0], sendbuf.shape[1]
    emb_count = xbuf.shape[1]
    y, x = dp % 4, dp // 4
    ring = (x * 4 + (y + 1) % 4, x * 4 + (y + 3) % 4, (x + 1) % 4 * 4 + y, (x + 3) % 4 * 4 + y)

    def peer(d, cc):
        return lax.rem(z + d, 8) * 2 + lax.rem(c + cc, 2)

    def load(s):
        part = pl.ds(s * group, group)
        return pltpu.make_async_copy(emb_ref.at[:, part], ebuf.at[:, part], load_sem.at[s])

    load(0).start()

    def place(chip):
        return jnp.where(chip == 7, 11, 2 * chip)

    def first(d, cc):
        return c == jnp.minimum(z, 1) if d == 0 else place(peer(d, cc) // 2) < place(z)

    def signal(semaphore, device):
        pl.semaphore_signal(semaphore, inc=1, device_id=device, device_id_type=MESH)

    half = 4
    late = z >= half

    def apart(d, cc):
        return jnp.logical_and(late, peer(d, cc) >= 2 * half) if d in (2, 3, 5, 6) else False

    barrier = pltpu.get_barrier_semaphore()
    heard = 2 * jnp.where(late, half + jnp.where(z == half + 1, 1, jnp.where(z == half + 2, 2, 0)), z) + (c == jnp.minimum(z, 1)).astype(jnp.int32)
    for d, cc in PEERS:
        pl.when(jnp.logical_not(jnp.logical_or(first(d, cc), apart(d, cc))))(functools.partial(signal, barrier, {"emb": peer(d, cc)}))
    answers = 0
    for k in range(4):
        pl.when(ring[k] > dp)(functools.partial(signal, barrier, {"dp": ring[k]}))
        heard = heard + (ring[k] < dp).astype(jnp.int32)
        answers = answers + (ring[k] > dp).astype(jnp.int32)

    my_w = pl.ds(pl.multiple_of(dp * rows, rows), rows)
    my_half = pl.ds(pl.multiple_of(c * (emb_count // 2), 128), emb_count // 2)
    own_w = pltpu.make_async_copy(w_ref.at[:, my_half], wfull.at[my_w, my_half], small_sem.at[0])
    own_w.start()
    for s in range(1, chunks):
        load(s).start()
    small = [
        pltpu.make_async_copy(a, v, small_sem.at[1])
        for i, (a, v) in enumerate(((mp_ref, wfull.at[pl.ds(emb_count, mp_ref.shape[0])]), (wf_ref, wf_v), (g_ref, g_v), (b_ref, b_v)))
    ]
    for copy in small:
        copy.start()

    pl.when(heard > 0)(lambda: pl.semaphore_wait(barrier, heard))
    for d, cc in PEERS:
        pl.when(jnp.logical_and(first(d, cc), jnp.logical_not(apart(d, cc))))(functools.partial(signal, ready.at[e], {"emb": peer(d, cc)}))
    for k in range(4):
        pl.when(ring[k] < dp)(functools.partial(signal, dp_ready, {"dp": ring[k]}))

    my_rows = pl.ds(pl.multiple_of(e * rows, rows), rows)

    def prepare(s):
        load(s).wait()
        for n in range(rows):
            block = ebuf[n, pl.ds(pl.multiple_of(s * group, group), group), :].astype(jnp.float32)
            for h in range(2):
                stage[h, pl.ds(n * PITCH, group), :] = block[:, h * 128 : (h + 1) * 128]
        for b in range(group):
            for h in range(2):
                sendbuf[s, b, :, pl.ds(h * 128, 128)] = stage[h, pl.ds(b, rows, stride=PITCH), :].astype(jnp.bfloat16)
        xbuf[s, my_rows, :] = sendbuf[s, e]

    def send_one(s, j):
        pltpu.make_async_remote_copy(
            src_ref=sendbuf.at[s, j], dst_ref=xbuf.at[s, my_rows],
            send_sem=in_send, recv_sem=in_recv.at[s],
            device_id={"emb": j}, device_id_type=MESH,
        ).start()

    def send_to(s, to_late, to_early):
        for d, cc in PEERS:
            if to_late and to_early:
                send_one(s, peer(d, cc))
            else:
                pl.when((peer(d, cc) >= 2 * half) == to_late)(functools.partial(send_one, s, peer(d, cc)))

    def await_peer(d, cc):
        pl.when(jnp.logical_not(first(d, cc)))(lambda: pl.semaphore_wait(ready.at[peer(d, cc)], 1))

    def w_copy(i, to, start, size):
        part = pl.ds(pl.multiple_of(start, 16), size)
        return pltpu.make_async_remote_copy(
            src_ref=wfull.at[part, my_half], dst_ref=wfull.at[part, my_half], send_sem=w_send, recv_sem=w_recv.at[i // 2],
            device_id={"dp": ring[to]}, device_id_type=MESH,
        )

    column = x * 4 * rows
    w_copies = (
        w_copy(0, 0, column + y * rows, rows),
        w_copy(1, 1, column + y * rows, rows),
        w_copy(2, 0, column + (y + 3) % 4 * rows, rows // 2),
        w_copy(3, 1, column + (y + 1) % 4 * rows + rows // 2, rows // 2),
        w_copy(4, 2, column, 4 * rows),
        w_copy(5, 3, column, 4 * rows),
        w_copy(6, 2, (x + 3) % 4 * 4 * rows, 2 * rows),
        w_copy(7, 3, (x + 1) % 4 * 4 * rows + 2 * rows, 2 * rows),
    )

    def start_weights():
        own_w.wait()
        pl.when(answers > 0)(lambda: pl.semaphore_wait(dp_ready, answers))
        w_copies[0].start()
        w_copies[1].start()

    @pl.when(jnp.logical_not(late))
    def _():
        def ready_made(s, carry):
            prepare(s)
            return carry

        lax.fori_loop(0, chunks, ready_made, 0)
        for d, cc in PEERS:

            @pl.when(peer(d, cc) < 2 * half)
            def _(d=d, cc=cc):
                await_peer(d, cc)
                for s in range(4):
                    send_one(s, peer(d, cc))

        start_weights()
        for d, cc in PEERS:

            @pl.when(peer(d, cc) >= 2 * half)
            def _(d=d, cc=cc):
                await_peer(d, cc)
                send_one(0, peer(d, cc))

        send_to(1, True, False)
        send_to(2, True, False)
        send_to(3, True, False)

    @pl.when(late)
    def _():
        for s in range(2):
            prepare(s)
            send_to(s, False, True)
        for s in range(2, 4):
            prepare(s)

        def tell(d, about):
            signal(told.at[about - half], {"emb": peer(d, 0)})

        for d, cc in PEERS[:5]:

            @pl.when(peer(d, cc) >= 2 * half)
            def _(d=d, cc=cc):
                await_peer(d, cc)
                send_one(0, peer(d, cc))

        @pl.when(jnp.logical_and(z > half, z < 7))
        def _():
            tell(1, z - 1)
            tell(7, z + 1)

        start_weights()
        for d in (6, 2, 5, 3):
            about = lax.rem(z + d, 8)

            @pl.when(apart(d, 0))
            def _(d=d, about=about):
                pl.semaphore_wait(told.at[about - half], 1)
                if d == 6:
                    pl.when(z == half + 2)(lambda: tell(1, about))
                if d == 2:
                    pl.when(z == half + 1)(lambda: tell(7, about))
                for cc in range(2):
                    send_one(0, peer(d, cc))

        send_to(1, True, False)
        send_to(2, True, True)
        send_to(3, True, True)

    for i in (0, 2, 4, 6):
        both = pl.ds(0, rows * (2, 1, 8, 4)[i // 2] // 2)
        pltpu.make_async_copy(wfull.at[both], wfull.at[both], w_recv.at[i // 2]).wait()
        if i < 6:
            w_copies[i + 2].start()
            w_copies[i + 3].start()
    whole = pl.ds(0, emb_count)
    swap = pltpu.make_async_remote_copy(
        src_ref=wfull.at[whole, my_half], dst_ref=wfull.at[whole, my_half], send_sem=w_send, recv_sem=w_recv.at[4],
        device_id={"emb": peer(0, 1)}, device_id_type=MESH,
    )
    swap.start()
    loaded = pl.ds(0, 7 * rank // 2)
    pltpu.make_async_copy(wfull.at[loaded], wfull.at[loaded], small_sem.at[1]).wait()
    swap.wait_recv()
    others = pl.ds(0, emb_count - rows)

    block = 128
    entries = jnp.float32(emb_count * width)

    def out_one(s, j):
        pltpu.make_async_remote_copy(
            src_ref=rbuf.at[s, pl.ds(pl.multiple_of(j * rows, rows), rows)], dst_ref=ybuf.at[s, e],
            send_sem=out_send, recv_sem=out_recv.at[s],
            device_id={"emb": j}, device_id_type=MESH,
        ).start()

    def send_out(s):
        def relative():
            for d, cc in PEERS:
                out_one(s, peer(d, cc))

        pl.when(s < 2)(relative)

    def mix(s, carry):
        pltpu.make_async_copy(xbuf.at[s, others], xbuf.at[s, others], in_recv.at[s]).wait()
        x = xbuf[s]
        factor = jnp.dot(wfull[pl.ds(emb_count, 32), :], x, preferred_element_type=jnp.float32).astype(jnp.bfloat16)
        total = jnp.zeros((8, width), jnp.float32)
        for i in range(emb_count // block):
            part = pl.ds(i * block, block)
            xb = xbuf[s, part, :]
            inner = lax.dot_general(xb, factor, (((1,), (1,)), ((), ())), preferred_element_type=jnp.float32).astype(jnp.bfloat16)
            m = jnp.dot(wfull[part, :], x, preferred_element_type=jnp.float32)
            m = m + xb.astype(jnp.float32) + jnp.dot(inner, wf_v[...], preferred_element_type=jnp.float32)
            mixed[part, :] = m
            total = total + jnp.sum(m.reshape(block // 8, 8, width), axis=0)
        average = jnp.sum(total, keepdims=True) / entries
        square = jnp.zeros((8, width), jnp.float32)
        for i in range(emb_count // block):
            centered = mixed[pl.ds(i * block, block), :] - average
            square = square + jnp.sum((centered * centered).reshape(block // 8, 8, width), axis=0)
        scale = lax.rsqrt(jnp.sum(square, keepdims=True) / entries + 1e-05)
        for i in range(emb_count // block):
            part = pl.ds(i * block, block)
            rbuf[s, part, :] = ((mixed[part, :] - average) * scale).astype(jnp.bfloat16)
        ybuf[s, e] = rbuf[s, my_rows, :]
        send_out(s)
        return carry

    lax.fori_loop(0, chunks, mix, 0)
    held = jnp.logical_and(z > 0, jnp.logical_not(late))
    second = jnp.logical_and(z == 0, c == 1)

    @pl.when(z > 0)
    def _():
        for chip, parts in ((2, (2,)), (1, (2,)), (0, (2, 3)), (1, (3,)), (2, (3,)), (3, (2, 3)), (4, (2, 3)), (5, (2, 3)), (6, (2, 3)), (7, (2, 3))):
            for j in (2 * chip, 2 * chip + 1):

                @pl.when(jnp.logical_and(j != e, jnp.logical_not(held)) if j in (12, 13, 14, 15) else j != e)
                def _(j=j, parts=parts):
                    for s in parts:
                        out_one(s, j)

    @pl.when(z == 0)
    def _():
        for chip in (5, 6, 7, 4, 1, 2, 3, 0):
            for j in (2 * chip, 2 * chip + 1):

                @pl.when(jnp.logical_and(j != e, jnp.logical_not(second)) if chip in (7,) else j != e)
                def _(j=j):
                    for s in range(2, 4):
                        out_one(s, j)


    fifteen = pl.ds(0, group - 1)

    def finish(s, carry):
        pltpu.make_async_copy(ybuf.at[s, fifteen], ybuf.at[s, fifteen], out_recv.at[s]).wait()

        @pl.when(jnp.logical_and(held, s == 1))
        def _():
            for j in (12, 13, 14, 15):
                for t in range(2, 4):
                    out_one(t, j)

        @pl.when(jnp.logical_and(second, s == 1))
        def _():
            for chip in (7,):
                for j in (2 * chip, 2 * chip + 1):
                    for t in range(2, 4):
                        out_one(t, j)

        part = pl.ds(pl.multiple_of(s * group, group), group)
        for b in range(group):
            y = ybuf[s, b].astype(jnp.float32) * g_v[...] + b_v[...]
            for h in range(2):
                stage[h, pl.ds(b, rows, stride=PITCH), :] = y[:, h * 128 : (h + 1) * 128]
        for n in range(rows):
            for h in range(2):
                out_ref[n, part, pl.ds(h * 128, 128)] = stage[h, pl.ds(n * PITCH, group), :].astype(jnp.bfloat16)
        return carry

    lax.fori_loop(0, chunks, finish, 0)

    sent = pltpu.make_async_copy(sendbuf.at[:, fifteen], sendbuf.at[:, fifteen], in_send)
    sent.wait()
    sent = pltpu.make_async_copy(ybuf.at[:, fifteen], ybuf.at[:, fifteen], out_send)
    sent.wait()
    passed = pl.ds(0, emb_count - rows // 2)
    pltpu.make_async_copy(wfull.at[passed], wfull.at[passed], w_send).wait()


def body(embeddings, machine_projection, w_lcb, w_fmb, ln_gain, ln_bias):
    rows, samples, width = embeddings.shape
    emb_count, rank = machine_projection.shape
    group = emb_count // rows
    chunks = samples // group
    hbm = pl.BlockSpec(memory_space=pltpu.HBM)
    operands = (embeddings, machine_projection.T, w_lcb, w_fmb, ln_gain, ln_bias)
    bf16, f32 = jnp.bfloat16, jnp.float32
    return pl.pallas_call(
        kernel,
        out_shape=pltpu.VMEM((rows, samples, width), bf16),
        in_specs=[hbm] * 6,
        out_specs=pl.BlockSpec(memory_space=pltpu.VMEM),
        scratch_shapes=[
            pltpu.VMEM((rows, samples, width), bf16),
            pltpu.VMEM((2, rows * PITCH, 128), f32),
            pltpu.VMEM((chunks, group, rows, width), bf16),
            pltpu.VMEM((chunks, emb_count, width), bf16),
            pltpu.VMEM((emb_count + rank, emb_count), bf16),
            pltpu.VMEM((chunks, emb_count, width), bf16),
            pltpu.VMEM((chunks, group, rows, width), bf16),
            pltpu.VMEM((emb_count, width), f32),
            pltpu.VMEM(w_fmb.shape, bf16),
            pltpu.VMEM(ln_gain.shape, f32),
            pltpu.VMEM(ln_bias.shape, f32),
            pltpu.SemaphoreType.DMA((chunks,)),
            pltpu.SemaphoreType.DMA((2,)),
            pltpu.SemaphoreType.DMA,
            pltpu.SemaphoreType.DMA((chunks,)),
            pltpu.SemaphoreType.DMA,
            pltpu.SemaphoreType.DMA((chunks,)),
            pltpu.SemaphoreType.DMA,
            pltpu.SemaphoreType.DMA((5,)),
            pltpu.SemaphoreType.REGULAR((group,)),
            pltpu.SemaphoreType.REGULAR,
            pltpu.SemaphoreType.REGULAR((4,)),
        ],
        compiler_params=pltpu.CompilerParams(
            collective_id=0, has_side_effects=True, vmem_limit_bytes=48 << 20
        ),
        name="wukong",
    )(*(pltpu.with_memory_space_constraint(a, pltpu.HBM) for a in operands))


def solution(mesh):
    placed = (P("emb", "dp", None), P(), P("dp", None), P(), P("emb", None), P("emb", None))
    return jax.shard_map(
        body, mesh=mesh, in_specs=placed, out_specs=P("emb", "dp", None), check_vma=False
    )
```

```python
import functools

import jax
import jax.numpy as jnp
from jax import lax
from jax.experimental import pallas as pl
from jax.experimental.pallas import tpu as pltpu
from jax.sharding import PartitionSpec as P

MESH = pl.DeviceIdType.MESH
PEERS = ((0, 1),) + tuple((d, c) for d in (1, 7, 2, 6, 3, 5, 4) for c in (0, 1))
PITCH = 24


def kernel(
    emb_ref, mp_ref, w_ref, wf_ref, g_ref, b_ref, out_ref,
    ebuf, stage, sendbuf, xbuf, wfull, rbuf, ybuf, mixed, wf_v, g_v, b_v,
    load_sem, small_sem, in_send, in_recv, out_send, out_recv, w_send, w_recv, ready, dp_ready, told,
):
    e = lax.axis_index("emb")
    dp = lax.axis_index("dp")
    z, c = e // 2, e % 2
    rows, samples, width = ebuf.shape
    rank = mp_ref.shape[0]
    chunks, group = sendbuf.shape[0], sendbuf.shape[1]
    emb_count = xbuf.shape[1]
    y, x = dp % 4, dp // 4
    ring = (x * 4 + (y + 1) % 4, x * 4 + (y + 3) % 4, (x + 1) % 4 * 4 + y, (x + 3) % 4 * 4 + y)

    def peer(d, cc):
        return lax.rem(z + d, 8) * 2 + lax.rem(c + cc, 2)

    def load(s):
        part = pl.ds(s * group, group)
        return pltpu.make_async_copy(emb_ref.at[:, part], ebuf.at[:, part], load_sem.at[s])

    load(0).start()

    def place(chip):
        return jnp.where(chip == 7, 11, 2 * chip)

    def first(d, cc):
        return c == jnp.minimum(z, 1) if d == 0 else place(peer(d, cc) // 2) < place(z)

    def signal(semaphore, device):
        pl.semaphore_signal(semaphore, inc=1, device_id=device, device_id_type=MESH)

    half = 4
    late = z >= half

    def apart(d, cc):
        return jnp.logical_and(late, peer(d, cc) >= 2 * half) if d in (2, 3, 5, 6) else False

    barrier = pltpu.get_barrier_semaphore()
    heard = 2 * jnp.where(late, half + jnp.where(z == half + 1, 1, jnp.where(z == half + 2, 2, 0)), z) + (c == jnp.minimum(z, 1)).astype(jnp.int32)
    for d, cc in PEERS:
        pl.when(jnp.logical_not(jnp.logical_or(first(d, cc), apart(d, cc))))(functools.partial(signal, barrier, {"emb": peer(d, cc)}))
    answers = 0
    for k in range(4):
        pl.when(ring[k] > dp)(functools.partial(signal, barrier, {"dp": ring[k]}))
        heard = heard + (ring[k] < dp).astype(jnp.int32)
        answers = answers + (ring[k] > dp).astype(jnp.int32)

    my_w = pl.ds(pl.multiple_of(dp * rows, rows), rows)
    my_half = pl.ds(pl.multiple_of(c * (emb_count // 2), 128), emb_count // 2)
    own_w = pltpu.make_async_copy(w_ref.at[:, my_half], wfull.at[my_w, my_half], small_sem.at[0])
    own_w.start()
    for s in range(1, chunks):
        load(s).start()
    small = [
        pltpu.make_async_copy(a, v, small_sem.at[1])
        for i, (a, v) in enumerate(((mp_ref, wfull.at[pl.ds(emb_count, mp_ref.shape[0])]), (wf_ref, wf_v), (g_ref, g_v), (b_ref, b_v)))
    ]
    for copy in small:
        copy.start()

    pl.when(heard > 0)(lambda: pl.semaphore_wait(barrier, heard))
    for d, cc in PEERS:
        pl.when(jnp.logical_and(first(d, cc), jnp.logical_not(apart(d, cc))))(functools.partial(signal, ready.at[e], {"emb": peer(d, cc)}))
    for k in range(4):
        pl.when(ring[k] < dp)(functools.partial(signal, dp_ready, {"dp": ring[k]}))

    my_rows = pl.ds(pl.multiple_of(e * rows, rows), rows)

    def arrange(s, blocks):
        for b in blocks:
            for h in range(2):
                sendbuf[s, b, :, pl.ds(h * 128, 128)] = stage[h, pl.ds(b, rows, stride=PITCH), :].astype(jnp.bfloat16)

    def stage_in(s):
        load(s).wait()
        for n in range(rows):
            block = ebuf[n, pl.ds(pl.multiple_of(s * group, group), group), :].astype(jnp.float32)
            for h in range(2):
                stage[h, pl.ds(n * PITCH, group), :] = block[:, h * 128 : (h + 1) * 128]

    def prepare(s):
        stage_in(s)
        arrange(s, range(group))
        xbuf[s, my_rows, :] = sendbuf[s, e]

    def send_one(s, j):
        pltpu.make_async_remote_copy(
            src_ref=sendbuf.at[s, j], dst_ref=xbuf.at[s, my_rows],
            send_sem=in_send, recv_sem=in_recv.at[s],
            device_id={"emb": j}, device_id_type=MESH,
        ).start()

    def send_to(s, to_late, to_early):
        for d, cc in PEERS:
            if to_late and to_early:
                send_one(s, peer(d, cc))
            else:
                pl.when((peer(d, cc) >= 2 * half) == to_late)(functools.partial(send_one, s, peer(d, cc)))

    def await_peer(d, cc):
        pl.when(jnp.logical_not(first(d, cc)))(lambda: pl.semaphore_wait(ready.at[peer(d, cc)], 1))

    def w_copy(i, to, start, size):
        part = pl.ds(pl.multiple_of(start, 16), size)
        return pltpu.make_async_remote_copy(
            src_ref=wfull.at[part, my_half], dst_ref=wfull.at[part, my_half], send_sem=w_send, recv_sem=w_recv.at[i // 2],
            device_id={"dp": ring[to]}, device_id_type=MESH,
        )

    column = x * 4 * rows
    w_copies = (
        w_copy(0, 0, column + y * rows, rows),
        w_copy(1, 1, column + y * rows, rows),
        w_copy(2, 0, column + (y + 3) % 4 * rows, rows // 2),
        w_copy(3, 1, column + (y + 1) % 4 * rows + rows // 2, rows // 2),
        w_copy(4, 2, column, 4 * rows),
        w_copy(5, 3, column, 4 * rows),
        w_copy(6, 2, (x + 3) % 4 * 4 * rows, 2 * rows),
        w_copy(7, 3, (x + 1) % 4 * 4 * rows + 2 * rows, 2 * rows),
    )

    def start_weights():
        own_w.wait()
        pl.when(answers > 0)(lambda: pl.semaphore_wait(dp_ready, answers))
        w_copies[0].start()
        w_copies[1].start()

    @pl.when(jnp.logical_not(late))
    def _():
        def ready_made(s, carry):
            prepare(s)
            return carry

        lax.fori_loop(0, chunks, ready_made, 0)
        for d, cc in PEERS:

            @pl.when(peer(d, cc) < 2 * half)
            def _(d=d, cc=cc):
                await_peer(d, cc)
                for s in range(4):
                    send_one(s, peer(d, cc))

        start_weights()
        for d, cc in PEERS:

            @pl.when(peer(d, cc) >= 2 * half)
            def _(d=d, cc=cc):
                await_peer(d, cc)
                send_one(0, peer(d, cc))

        send_to(1, True, False)
        send_to(2, True, False)
        send_to(3, True, False)

    @pl.when(late)
    def _():
        stage_in(0)
        arrange(0, range(2 * half))
        send_to(0, False, True)
        arrange(0, range(2 * half, group))
        xbuf[0, my_rows, :] = sendbuf[0, e]
        prepare(1)
        send_to(1, False, True)
        for s in range(2, 4):
            prepare(s)

        def tell(d, about):
            signal(told.at[about - half], {"emb": peer(d, 0)})

        for d, cc in PEERS[:5]:

            @pl.when(peer(d, cc) >= 2 * half)
            def _(d=d, cc=cc):
                await_peer(d, cc)
                send_one(0, peer(d, cc))

        @pl.when(jnp.logical_and(z > half, z < 7))
        def _():
            tell(1, z - 1)
            tell(7, z + 1)

        start_weights()
        for d in (6, 2, 5, 3):
            about = lax.rem(z + d, 8)

            @pl.when(apart(d, 0))
            def _(d=d, about=about):
                pl.semaphore_wait(told.at[about - half], 1)
                if d == 6:
                    pl.when(z == half + 2)(lambda: tell(1, about))
                if d == 2:
                    pl.when(z == half + 1)(lambda: tell(7, about))
                for cc in range(2):
                    send_one(0, peer(d, cc))

        send_to(1, True, False)
        send_to(2, True, True)
        send_to(3, True, True)

    for i in (0, 2, 4, 6):
        both = pl.ds(0, rows * (2, 1, 8, 4)[i // 2] // 2)
        pltpu.make_async_copy(wfull.at[both], wfull.at[both], w_recv.at[i // 2]).wait()
        if i < 6:
            w_copies[i + 2].start()
            w_copies[i + 3].start()
    whole = pl.ds(0, emb_count)
    swap = pltpu.make_async_remote_copy(
        src_ref=wfull.at[whole, my_half], dst_ref=wfull.at[whole, my_half], send_sem=w_send, recv_sem=w_recv.at[4],
        device_id={"emb": peer(0, 1)}, device_id_type=MESH,
    )
    swap.start()
    loaded = pl.ds(0, 7 * rank // 2)
    pltpu.make_async_copy(wfull.at[loaded], wfull.at[loaded], small_sem.at[1]).wait()
    swap.wait_recv()
    others = pl.ds(0, emb_count - rows)

    block = 128
    entries = jnp.float32(emb_count * width)

    def out_one(s, j):
        pltpu.make_async_remote_copy(
            src_ref=rbuf.at[s, pl.ds(pl.multiple_of(j * rows, rows), rows)], dst_ref=ybuf.at[s, e],
            send_sem=out_send, recv_sem=out_recv.at[s],
            device_id={"emb": j}, device_id_type=MESH,
        ).start()

    def send_out(s):
        def relative():
            for d, cc in PEERS:
                out_one(s, peer(d, cc))

        pl.when(s < 2)(relative)

    def mix(s, carry):
        pltpu.make_async_copy(xbuf.at[s, others], xbuf.at[s, others], in_recv.at[s]).wait()
        x = xbuf[s]
        factor = jnp.dot(wfull[pl.ds(emb_count, 32), :], x, preferred_element_type=jnp.float32).astype(jnp.bfloat16)
        total = jnp.zeros((8, width), jnp.float32)
        for i in range(emb_count // block):
            part = pl.ds(i * block, block)
            xb = xbuf[s, part, :]
            inner = lax.dot_general(xb, factor, (((1,), (1,)), ((), ())), preferred_element_type=jnp.float32).astype(jnp.bfloat16)
            m = jnp.dot(wfull[part, :], x, preferred_element_type=jnp.float32)
            m = m + xb.astype(jnp.float32) + jnp.dot(inner, wf_v[...], preferred_element_type=jnp.float32)
            mixed[part, :] = m
            total = total + jnp.sum(m.reshape(block // 8, 8, width), axis=0)
        average = jnp.sum(total, keepdims=True) / entries
        square = jnp.zeros((8, width), jnp.float32)
        for i in range(emb_count // block):
            centered = mixed[pl.ds(i * block, block), :] - average
            square = square + jnp.sum((centered * centered).reshape(block // 8, 8, width), axis=0)
        scale = lax.rsqrt(jnp.sum(square, keepdims=True) / entries + 1e-05)
        for i in range(emb_count // block):
            part = pl.ds(i * block, block)
            rbuf[s, part, :] = ((mixed[part, :] - average) * scale).astype(jnp.bfloat16)
        ybuf[s, e] = rbuf[s, my_rows, :]
        send_out(s)
        return carry

    lax.fori_loop(0, chunks, mix, 0)
    held = jnp.logical_and(z > 0, jnp.logical_not(late))
    second = jnp.logical_and(z == 0, c == 1)

    @pl.when(z > 0)
    def _():
        for chip, parts in ((2, (2,)), (1, (2,)), (0, (2, 3)), (1, (3,)), (2, (3,)), (3, (2, 3)), (4, (2, 3)), (5, (2, 3)), (6, (2, 3)), (7, (2, 3))):
            for j in (2 * chip, 2 * chip + 1):

                @pl.when(jnp.logical_and(j != e, jnp.logical_not(held)) if j in (12, 13, 14, 15) else j != e)
                def _(j=j, parts=parts):
                    for s in parts:
                        out_one(s, j)

    @pl.when(z == 0)
    def _():
        for chip in (5, 6, 7, 4, 1, 2, 3, 0):
            for j in (2 * chip, 2 * chip + 1):

                @pl.when(jnp.logical_and(j != e, jnp.logical_not(second)) if chip in (7,) else j != e)
                def _(j=j):
                    for s in range(2, 4):
                        out_one(s, j)


    fifteen = pl.ds(0, group - 1)

    def finish(s, carry):
        pltpu.make_async_copy(ybuf.at[s, fifteen], ybuf.at[s, fifteen], out_recv.at[s]).wait()

        @pl.when(jnp.logical_and(held, s == 1))
        def _():
            for j in (12, 13, 14, 15):
                for t in range(2, 4):
                    out_one(t, j)

        @pl.when(jnp.logical_and(second, s == 1))
        def _():
            for chip in (7,):
                for j in (2 * chip, 2 * chip + 1):
                    for t in range(2, 4):
                        out_one(t, j)

        part = pl.ds(pl.multiple_of(s * group, group), group)
        for b in range(group):
            y = ybuf[s, b].astype(jnp.float32) * g_v[...] + b_v[...]
            for h in range(2):
                stage[h, pl.ds(b, rows, stride=PITCH), :] = y[:, h * 128 : (h + 1) * 128]
        for n in range(rows):
            for h in range(2):
                out_ref[n, part, pl.ds(h * 128, 128)] = stage[h, pl.ds(n * PITCH, group), :].astype(jnp.bfloat16)
        return carry

    lax.fori_loop(0, chunks, finish, 0)

    sent = pltpu.make_async_copy(sendbuf.at[:, fifteen], sendbuf.at[:, fifteen], in_send)
    sent.wait()
    sent = pltpu.make_async_copy(ybuf.at[:, fifteen], ybuf.at[:, fifteen], out_send)
    sent.wait()
    passed = pl.ds(0, emb_count - rows // 2)
    pltpu.make_async_copy(wfull.at[passed], wfull.at[passed], w_send).wait()


def body(embeddings, machine_projection, w_lcb, w_fmb, ln_gain, ln_bias):
    rows, samples, width = embeddings.shape
    emb_count, rank = machine_projection.shape
    group = emb_count // rows
    chunks = samples // group
    hbm = pl.BlockSpec(memory_space=pltpu.HBM)
    operands = (embeddings, machine_projection.T, w_lcb, w_fmb, ln_gain, ln_bias)
    bf16, f32 = jnp.bfloat16, jnp.float32
    return pl.pallas_call(
        kernel,
        out_shape=pltpu.VMEM((rows, samples, width), bf16),
        in_specs=[hbm] * 6,
        out_specs=pl.BlockSpec(memory_space=pltpu.VMEM),
        scratch_shapes=[
            pltpu.VMEM((rows, samples, width), bf16),
            pltpu.VMEM((2, rows * PITCH, 128), f32),
            pltpu.VMEM((chunks, group, rows, width), bf16),
            pltpu.VMEM((chunks, emb_count, width), bf16),
            pltpu.VMEM((emb_count + rank, emb_count), bf16),
            pltpu.VMEM((chunks, emb_count, width), bf16),
            pltpu.VMEM((chunks, group, rows, width), bf16),
            pltpu.VMEM((emb_count, width), f32),
            pltpu.VMEM(w_fmb.shape, bf16),
            pltpu.VMEM(ln_gain.shape, f32),
            pltpu.VMEM(ln_bias.shape, f32),
            pltpu.SemaphoreType.DMA((chunks,)),
            pltpu.SemaphoreType.DMA((2,)),
            pltpu.SemaphoreType.DMA,
            pltpu.SemaphoreType.DMA((chunks,)),
            pltpu.SemaphoreType.DMA,
            pltpu.SemaphoreType.DMA((chunks,)),
            pltpu.SemaphoreType.DMA,
            pltpu.SemaphoreType.DMA((5,)),
            pltpu.SemaphoreType.REGULAR((group,)),
            pltpu.SemaphoreType.REGULAR,
            pltpu.SemaphoreType.REGULAR((4,)),
        ],
        compiler_params=pltpu.CompilerParams(
            collective_id=0, has_side_effects=True, vmem_limit_bytes=48 << 20
        ),
        name="wukong",
    )(*(pltpu.with_memory_space_constraint(a, pltpu.HBM) for a in operands))


def solution(mesh):
    placed = (P("emb", "dp", None), P(), P("dp", None), P(), P("emb", None), P("emb", None))
    return jax.shard_map(
        body, mesh=mesh, in_specs=placed, out_specs=P("emb", "dp", None), check_vma=False
    )
```
